32 devices in a mesh: groups: 2 (over y), space: 4 (over z), mp: 2 (over x), sub: 2 (over core).
Axes of the slice: x: 2, y: 2, z: 4, core: 2. Of those that a mesh axis runs over, the one named last changes fastest.
Arguments:
- voxels: bfloat16 [24576, 512], P(('groups', 'space', 'sub')), parts along dimension 0, may hold values from -6 to 6
- window_ids: int32 [24576], P(('groups', 'space', 'sub')), parts along dimension 0, may hold values from 0 to 127, as said below
- voxel_slots: int32 [24576], P(('groups', 'space', 'sub')), parts along dimension 0, may hold values from 0 to 255, as said below
- window_counts: int32 [256], P('groups'), parts along dimension 0, may hold values from 0 to 256, as said below
- norm_gain: float32 [512], replicated, may hold values from 0.25 to 1.75
- w_query_key: bfloat16 [2, 512, 512], P(None, None, 'mp'), may hold values from -2 to 2
- w_value: bfloat16 [512, 512], P(None, 'mp'), may hold values from -0.25 to 0.25
- w_out: bfloat16 [512, 512], P('mp'), may hold values from -0.25 to 0.25
- ffn_gain: float32 [512], replicated, may hold values from 0.25 to 1.75
- w_up: bfloat16 [512, 2048], P(None, 'mp'), may hold values from -0.25 to 0.25
- w_down: bfloat16 [2048, 512], P('mp'), may hold values from -0.125 to 0.125
Outputs:
- result: bfloat16 [24576, 512], P(('groups', 'space', 'sub'), 'mp'), parts along dimension 0
The draws below stay inside these ranges and needn't reach their ends.
There are 2 independent parts, one for each index of `groups`. The reference program is written for one: setup_inputs(seed, part) draws one part's arguments, and reference() takes and returns one part's arrays. A program takes and returns all parts, laid end to end along the dimension named above; an argument that names none is the same for every part. Nothing has to cross between parts.
Inputs may be any that keep to these rules, and one draw needn't show every extreme that they name: `window_ids`: window w belongs to owner w // 16 (its index along space+sub) as that owner's window w % 16. On the voxels of one device at most 384 lie in windows of one owner, and in every draw some owner has exactly 384 voxels of every device. `voxel_slots`: the voxels of a window hold slots 0 to its count - 1, each once. window_counts[w] is the number of voxels with window id w; some window holds 256.
All inputs are finite; a program needn't handle non-finite values.
Results may differ from the reference program's by a relative error of at most 0.012.
Values may be sent and summed in bfloat16 or wider, within the bound.
A program may use at most 128 MiB of HBM per device.

```python
import jax
import jax.numpy as jnp
from jax import lax

D = 512
HEADS = 8
HDIM = 64
FF = 2048
WLEN = 256
VOX_DEV = 1536
NOWN = 8
VOX = 12288
CAP = 384
WIN_DEV = 16
NWIN = 128


def scene(key):
    owner_total = NOWN
    capacity = CAP
    per_owner = WIN_DEV
    key_bias = jax.random.fold_in(key, 101)
    key_first = jax.random.fold_in(key, 102)
    key_score = jax.random.fold_in(key, 103)
    key_shuffle = jax.random.fold_in(key, 104)
    key_sizes = jax.random.fold_in(key, 105)
    bias = jax.random.randint(key_bias, (owner_total,), 0, 3)
    busiest = jax.random.randint(key_first, (), 0, owner_total)
    bias = jnp.where(jnp.arange(owner_total) == busiest, 3, bias)
    scores = jax.random.randint(key_score, (owner_total, owner_total, capacity), 0, 1 << 20) + (bias * (1 << 20))[None, :, None]
    scores = scores.reshape(owner_total, owner_total * capacity)
    chosen = jnp.argsort(-scores, axis=1, stable=True)[:, :VOX_DEV].astype(jnp.int32)
    source_ids = jnp.arange(owner_total, dtype=jnp.int32)[:, None]
    selected = jnp.zeros((owner_total, owner_total * capacity), jnp.int32).at[source_ids, chosen].set(1)
    shuffles = jax.vmap(lambda sub_key: jax.random.permutation(sub_key, VOX_DEV))(jax.random.split(key_shuffle, owner_total))
    slot_ids = jnp.take_along_axis(chosen, shuffles.astype(jnp.int32), axis=1)
    owner_of = slot_ids // capacity
    column_of = slot_ids % capacity
    by_owner = selected.reshape(owner_total, owner_total, capacity).transpose(1, 0, 2).reshape(owner_total, owner_total * capacity)
    earlier = (jnp.cumsum(by_owner, axis=1) - by_owner).reshape(owner_total, owner_total, capacity)
    rank_of = earlier[owner_of, jnp.broadcast_to(source_ids, owner_of.shape), column_of]
    sizes = jax.random.randint(key_sizes, (owner_total, per_owner), 3 * WLEN // 4, WLEN + 1)
    sizes = sizes.at[:, 0].set(WLEN)
    ends = jnp.cumsum(sizes, axis=1)
    starts = ends - sizes
    local_win = jnp.sum((rank_of[:, :, None] >= ends[owner_of]).astype(jnp.int32), axis=-1)
    slot_in = rank_of - jnp.take_along_axis(starts[owner_of], local_win[:, :, None], axis=-1)[:, :, 0]
    load = jnp.sum(selected.reshape(owner_total, owner_total, capacity), axis=(0, 2))
    counts_flat = jnp.clip(load[:, None] - starts, 0, sizes).reshape(-1)
    window_of = owner_of * per_owner + local_win
    return (window_of.reshape(-1).astype(jnp.int32), slot_in.reshape(-1).astype(jnp.int32), counts_flat.astype(jnp.int32))


def draw_window_ids(key, part):
    return scene(key)[0]


def draw_voxel_slots(key, part):
    return scene(key)[1]


def draw_window_counts(key, part):
    return scene(key)[2]


def draw_w_query_key(key, part):
    key_base = jax.random.fold_in(key, 201)
    stacked = jax.random.normal(key_base, (2, D, D), jnp.float32) * D ** (-0.5)
    return jnp.clip(stacked, -2.0, 2.0).astype(jnp.bfloat16)


def block_scale(rng, dims, pieces, low, high):
    factor_of, own = 1.0, jax.random.fold_in(rng, 6)
    for axis_at, shards_of in pieces:
        heights = jnp.exp(jax.random.uniform(jax.random.fold_in(own, axis_at), (shards_of,), jnp.float32, low / len(pieces), high / len(pieces)))
        factor_of = factor_of * jnp.repeat(heights, dims[axis_at] // shards_of).reshape([-1 if axis == axis_at else 1 for axis in range(len(dims))])
    return factor_of


def scatter_about(stream_key, dims, deviation, limit, pieces=(), kind=jnp.bfloat16):
    values = jax.random.normal(stream_key, dims, jnp.float32) * deviation
    if len(pieces) > 0:
        values = block_scale(stream_key, dims, pieces, -0.22, 0.18) * values
    return jnp.clip(values, min=-limit, max=limit).astype(kind)


def setup_inputs(seed: int = 0, part: int = 0) -> dict:
    splits = jax.random.split(jax.random.key(seed), 12)
    part_splits = jax.random.split(jax.random.fold_in(splits[11], part), 12)
    voxels = scatter_about(part_splits[0], (VOX, D), 1.0, 6.0, ((0, 8),))
    window_ids = draw_window_ids(jax.random.fold_in(jax.random.fold_in(splits[11], part), 71), part)
    voxel_slots = draw_voxel_slots(jax.random.fold_in(jax.random.fold_in(splits[11], part), 71), part)
    window_counts = draw_window_counts(jax.random.fold_in(jax.random.fold_in(splits[11], part), 71), part)
    norm_gain = jnp.clip(1.0 + 0.15 * jax.random.normal(splits[4], (D,), jnp.float32), 0.25, 1.75)
    w_query_key = draw_w_query_key(jax.random.fold_in(splits[11], 71), part)
    w_value = scatter_about(splits[6], (D, D), D ** -0.5, 0.25, ((1, 2),))
    w_out = scatter_about(splits[7], (D, D), D ** -0.5, 0.25, ((0, 2),))
    ffn_gain = jnp.clip(1.0 + 0.15 * jax.random.normal(splits[8], (D,), jnp.float32), 0.25, 1.75)
    w_up = scatter_about(splits[9], (D, FF), D ** -0.5, 0.25, ((1, 2),))
    w_down = scatter_about(splits[10], (FF, D), FF ** -0.5, 0.125, ((0, 2),))
    return dict(voxels=voxels, window_ids=window_ids, voxel_slots=voxel_slots, window_counts=window_counts, norm_gain=norm_gain, w_query_key=w_query_key, w_value=w_value, w_out=w_out, ffn_gain=ffn_gain, w_up=w_up, w_down=w_down)


def normalize(values_in, gain):
    row_mean = lax.optimization_barrier(jnp.mean(values_in, axis=-1, keepdims=True))
    centred = values_in - row_mean
    variance = lax.optimization_barrier(jnp.mean(centred * centred, axis=-1, keepdims=True))
    return centred * lax.rsqrt(variance + 1e-05) * gain.astype(jnp.float32)

def reference(voxels, window_ids, voxel_slots, window_counts, norm_gain, w_query_key, w_value, w_out, ffn_gain, w_up, w_down):
    stream = voxels.astype(jnp.float32)
    normed = normalize(stream, norm_gain).astype(jnp.bfloat16)
    queries = jnp.dot(normed, w_query_key[0], preferred_element_type=jnp.float32).astype(jnp.bfloat16)
    key_rows = jnp.dot(normed, w_query_key[1], preferred_element_type=jnp.float32).astype(jnp.bfloat16)
    values = jnp.dot(normed, w_value, preferred_element_type=jnp.float32).astype(jnp.bfloat16)
    flat_index = (window_ids * WLEN + voxel_slots).astype(jnp.int32)
    slot_table = jnp.zeros((NWIN * WLEN,), jnp.int32).at[flat_index].set(jnp.arange(VOX, dtype=jnp.int32))
    slot_table = slot_table.reshape(NWIN, WLEN)

    def one_window(operands):
        members, count = operands
        split_shape = (WLEN, HEADS, HDIM)
        window_q = queries[members].astype(jnp.float32).reshape(split_shape)
        window_k = key_rows[members].astype(jnp.float32).reshape(split_shape)
        window_v = values[members].astype(jnp.float32).reshape(split_shape)
        scores = jnp.einsum('qhd,khd->hqk', window_q, window_k, precision=lax.Precision.HIGHEST) * HDIM ** (-0.5)
        live_keys = jnp.arange(WLEN, dtype=jnp.int32) < count
        scores = jnp.where(live_keys[None, None, :], scores, jnp.float32(-1e+30))
        row_max = lax.optimization_barrier(jnp.max(scores, axis=-1, keepdims=True))
        weights = jnp.exp(scores - row_max)
        probabilities = (weights / lax.optimization_barrier(jnp.sum(weights, axis=-1, keepdims=True))).astype(jnp.bfloat16)
        mixture = jnp.einsum('hqk,khd->qhd', probabilities.astype(jnp.float32), window_v, precision=lax.Precision.HIGHEST)
        return mixture.astype(jnp.bfloat16).reshape(WLEN, D)
    windows_out = lax.map(one_window, (slot_table, window_counts))
    attended = windows_out.reshape(NWIN * WLEN, D)[flat_index]
    after_attn = stream + jnp.dot(attended, w_out, preferred_element_type=jnp.float32)
    normed_ffn = normalize(after_attn, ffn_gain).astype(jnp.bfloat16)
    hidden = jax.nn.gelu(jnp.dot(normed_ffn, w_up, preferred_element_type=jnp.float32), approximate=True).astype(jnp.bfloat16)
    return (after_attn + jnp.dot(hidden, w_down, preferred_element_type=jnp.float32)).astype(jnp.bfloat16)
```

```python
import functools
import math

import jax
import jax.numpy as jnp
from jax import lax
from jax.experimental import pallas as pl
from jax.experimental.pallas import tpu as pltpu
from jax.sharding import PartitionSpec as P

HDIM = 64
WLEN = 256
WIN_DEV = 16
BASE = 64
MESH = pl.DeviceIdType.MESH
VMEM = pl.BlockSpec(memory_space=pltpu.VMEM)
f32 = jnp.float32
bf16 = jnp.bfloat16


def normalize(values_in, gain):
    row_mean = jnp.mean(values_in, axis=-1, keepdims=True)
    centred = values_in - row_mean
    variance = jnp.mean(centred * centred, axis=-1, keepdims=True)
    return centred * lax.rsqrt(variance + 1e-05) * gain


def iota(shape, dim):
    return lax.broadcasted_iota(jnp.int32, shape, dim)


def one_hot(found):
    return jnp.where(found, f32(1), f32(0)).astype(bf16)


def dot(a, b, dims=((1,), (0,))):
    return lax.dot_general(a, b, (dims, ((), ())), preferred_element_type=f32)


def greet(owners, subs, mp_n, me, m):
    barrier = pltpu.get_barrier_semaphore()
    for k in range(1, owners):
        t = (me + k) % owners
        pl.semaphore_signal(
            barrier, inc=1, device_id={"space": t // subs, "sub": t % subs}, device_id_type=MESH
        )
    for p in range(1, mp_n):
        pl.semaphore_signal(
            barrier, inc=1, device_id={"mp": (m + p) % mp_n}, device_id_type=MESH
        )
    pl.semaphore_wait(barrier, owners - 1 + mp_n - 1)


def to_owner(src, dst, sems, slot, target, subs):
    return pltpu.make_async_remote_copy(
        src_ref=src,
        dst_ref=dst,
        send_sem=sems[0].at[slot],
        recv_sem=sems[1].at[slot],
        device_id={"space": target // subs, "sub": target % subs},
        device_id_type=MESH,
    )


def to_mp(src, dst, sems, index, peer):
    return pltpu.make_async_remote_copy(
        src_ref=src,
        dst_ref=dst,
        send_sem=sems[0].at[index],
        recv_sem=sems[1].at[index],
        device_id={"mp": peer},
        device_id_type=MESH,
    )


def relay(owners, subs, mp_n, me, m, outbuf, blocks, main, side):
    last = owners - 1

    def onward(slot, carry):
        s = (me + owners - slot - 1) % owners
        to_owner(outbuf.at[slot], blocks.at[m, s], main, slot, s, subs).wait_recv()
        for p in range(1, mp_n):
            to_mp(
                blocks.at[m, s], blocks.at[m, s], side, slot * (mp_n - 1) + p - 1, (m + p) % mp_n
            ).start()
        return carry

    for p in range(1, mp_n):
        to_mp(
            outbuf.at[last], blocks.at[m, me], side, last * (mp_n - 1) + p - 1, (m + p) % mp_n
        ).start()
    lax.fori_loop(0, last, onward, 0)

    def finish(slot, carry):
        s = (me + owners - slot - 1) % owners
        for p in range(1, mp_n):
            to_mp(
                outbuf.at[slot],
                blocks.at[(m + mp_n - p) % mp_n, s],
                side,
                slot * (mp_n - 1) + p - 1,
                (m + p) % mp_n,
            ).wait()
        return carry

    lax.fori_loop(0, owners, finish, 0)

    def sent(slot, carry):
        to_owner(outbuf.at[slot], blocks.at[m, me], main, slot, me, subs).wait_send()
        return carry

    lax.fori_loop(0, last, sent, 0)


def dispatch_kernel(
    owners, subs, mp_n, half, index, digits, out_rows, arrived, spots, whole_out,
    outbuf, spotbuf, ms, mr, ps, pr, ss, sr, ws, wr,
):
    me = lax.axis_index("space") * subs + lax.axis_index("sub")
    m = lax.axis_index("mp")
    cap, rows = outbuf.shape[1], half.shape[0]
    greet(owners, subs, mp_n, me, m)
    for p in range(1, mp_n):
        to_mp(out_rows, whole_out.at[m], (ws, wr), p - 1, (m + p) % mp_n).start()
    whole_out[m] = out_rows[...]

    def send(slot):
        t = (me + slot + 1) % owners
        to_owner(outbuf.at[slot], arrived.at[m, me], (ms, mr), slot, t, subs).start()
        to_owner(spotbuf.at[slot], spots.at[me], (ps, pr), slot, t, subs).start()

    def build(slot, carry):
        t = (me + slot + 1) % owners
        hit = one_hot(index[...] == iota((cap, rows), 0) + t * cap)
        outbuf[slot] = dot(hit, half[...]).astype(bf16)
        parts = dot(digits[...], hit, ((1,), (1,)))
        place = parts[0:1] * BASE + parts[1:2] + (1 - parts[2:3]) * (WIN_DEV * WLEN)
        spotbuf[slot] = place.astype(jnp.int32)

        @pl.when(slot > 0)
        def _():
            send(slot - 1)

        return carry

    lax.fori_loop(0, owners, build, 0)
    arrived[m, me] = outbuf[owners - 1]
    spots[me] = spotbuf[owners - 1]
    relay(owners, subs, mp_n, me, m, outbuf, arrived, (ms, mr), (ss, sr))

    def tail(slot, carry):
        s = (me + owners - slot - 1) % owners
        to_owner(spotbuf.at[slot], spots.at[s], (ps, pr), slot, s, subs).wait()
        return carry

    lax.fori_loop(0, owners - 1, tail, 0)
    for p in range(1, mp_n):
        to_mp(
            out_rows, whole_out.at[(m + mp_n - p) % mp_n], (ws, wr), p - 1, (m + p) % mp_n
        ).wait()


def dispatch(owners, subs, mp_n, cap, half, index, digits, out_rows):
    part = half.shape[1]
    dma = pltpu.SemaphoreType.DMA
    side = owners * (mp_n - 1)
    return pl.pallas_call(
        functools.partial(dispatch_kernel, owners, subs, mp_n),
        out_shape=(
            jax.ShapeDtypeStruct((mp_n, owners, cap, part), bf16),
            jax.ShapeDtypeStruct((owners, 1, cap), jnp.int32),
            jax.ShapeDtypeStruct((mp_n,) + out_rows.shape, bf16),
        ),
        in_specs=[VMEM] * 4,
        out_specs=(VMEM, VMEM, VMEM),
        scratch_shapes=[
            pltpu.VMEM((owners, cap, part), bf16),
            pltpu.VMEM((owners, 1, cap), jnp.int32),
            dma((owners,)), dma((owners,)), dma((owners,)), dma((owners,)),
            dma((side,)), dma((side,)), dma((mp_n,)), dma((mp_n,)),
        ],
        compiler_params=pltpu.CompilerParams(collective_id=0, has_side_effects=True),
        name="dispatch",
    )(half, index, digits, out_rows)


def attend_kernel(group, counts, spots, arrived, w_qk, w_v, mixture):
    step = pl.program_id(0)
    halves, total, part = arrived.shape
    local = w_v.shape[1]
    heads = local // HDIM
    slots = group * WLEN
    hit = one_hot(spots[...] == iota((slots, total), 0) + step * slots)
    rows_in = jnp.concatenate(
        [dot(hit, arrived[h]).astype(bf16) for h in range(halves)], axis=1
    )
    queries = dot(rows_in, w_qk[0]).astype(bf16)
    keys = dot(rows_in, w_qk[1]).astype(bf16)
    values = dot(rows_in, w_v[...]).astype(bf16)
    head_of = iota((1, local), 1) // HDIM
    masks = [jnp.where(head_of == h, f32(1), f32(0)).astype(bf16) for h in range(heads)]
    for g in range(group):
        span = slice(g * WLEN, (g + 1) * WLEN)
        q, k, v = queries[span], keys[span], values[span]
        stacked = jnp.concatenate([q * masks[h] for h in range(heads)], axis=0)
        scores = dot(stacked, k, ((1,), (1,))) * f32(HDIM ** -0.5)
        live = iota((1, WLEN), 1) < counts[step * group + g]
        scores = jnp.where(live, scores, f32(-1e30))
        weights = jnp.exp(scores - jnp.max(scores, axis=-1, keepdims=True))
        scale = 1.0 / jnp.sum(weights, axis=-1, keepdims=True)
        mixed = dot((weights * scale).astype(bf16), v)
        out = mixed[:WLEN]
        for h in range(1, heads):
            out = jnp.where(head_of == h, mixed[h * WLEN : (h + 1) * WLEN], out)
        mixture[span, :] = out.astype(bf16)


def attend(counts, spots, arrived, w_qk, w_v, group=2):
    local = w_v.shape[1]
    whole = lambda a: pl.BlockSpec(a.shape, lambda i: (0,) * a.ndim)
    return pl.pallas_call(
        functools.partial(attend_kernel, group),
        grid=(WIN_DEV // group,),
        out_shape=jax.ShapeDtypeStruct((WIN_DEV * WLEN, local), bf16),
        in_specs=[pl.BlockSpec(memory_space=pltpu.SMEM)]
        + [whole(a) for a in (spots, arrived, w_qk, w_v)],
        out_specs=pl.BlockSpec((group * WLEN, local), lambda i: (i, 0)),
        name="attend",
    )(counts, spots, arrived, w_qk, w_v)


def answer_kernel(owners, subs, mp_n, mixture, column, answers, outbuf, total, ms, mr, ss, sr):
    me = lax.axis_index("space") * subs + lax.axis_index("sub")
    m = lax.axis_index("mp")
    cap = outbuf.shape[1]
    span = 4 * WLEN
    greet(owners, subs, mp_n, me, m)

    def send(slot):
        t = (me + slot + 1) % owners
        to_owner(outbuf.at[slot], answers.at[m, me], (ms, mr), slot, t, subs).start()

    def build(slot, carry):
        t = (me + slot + 1) % owners
        place = column[t]
        total[...] = jnp.zeros_like(total)

        def add(c, inner):
            hit = one_hot(place == iota((cap, span), 1) + c * span)
            total[...] += dot(hit, mixture[pl.ds(c * span, span), :])
            return inner

        lax.fori_loop(0, mixture.shape[0] // span, add, 0)
        outbuf[slot] = total[...].astype(bf16)

        @pl.when(slot > 0)
        def _():
            send(slot - 1)

        return carry

    lax.fori_loop(0, owners, build, 0)
    answers[m, me] = outbuf[owners - 1]
    relay(owners, subs, mp_n, me, m, outbuf, answers, (ms, mr), (ss, sr))


def answer(owners, subs, mp_n, cap, mixture, column):
    local = mixture.shape[1]
    dma = pltpu.SemaphoreType.DMA
    side = owners * (mp_n - 1)
    return pl.pallas_call(
        functools.partial(answer_kernel, owners, subs, mp_n),
        out_shape=jax.ShapeDtypeStruct((mp_n, owners, cap, local), bf16),
        in_specs=[VMEM] * 2,
        out_specs=VMEM,
        scratch_shapes=[
            pltpu.VMEM((owners, cap, local), bf16),
            pltpu.VMEM((cap, local), f32),
            dma((owners,)), dma((owners,)), dma((side,)), dma((side,)),
        ],
        compiler_params=pltpu.CompilerParams(collective_id=1, has_side_effects=True),
        name="answer",
    )(mixture, column)


def pick(value, which, pieces):
    part = value.shape[1] // pieces
    out = value[:, :part]
    for j in range(1, pieces):
        out = jnp.where(which == j, value[:, j * part : (j + 1) * part], out)
    return out


def ffn_kernel(
    mp_n, block, voxels, index, answers, w_out, gain, w_up, w_down, result,
    sendbuf, recvbuf, mine, ss, sr,
):
    m = lax.axis_index("mp")
    rows = voxels.shape[0]
    steps = rows // block
    total = answers.shape[1]
    barrier = pltpu.get_barrier_semaphore()
    for p in range(1, mp_n):
        pl.semaphore_signal(
            barrier, inc=1, device_id={"mp": (m + p) % mp_n}, device_id_type=MESH
        )
    pl.semaphore_wait(barrier, mp_n - 1)

    def copy(b, p):
        span = pl.ds(b * block, block)
        return to_mp(
            sendbuf.at[p - 1, span], recvbuf.at[p - 1, span], (ss, sr),
            b * (mp_n - 1) + p - 1, (m + p) % mp_n,
        )

    def work(b, carry):
        span = pl.ds(b * block, block)
        hit = one_hot(index[span, :] == iota((block, total), 1))
        after = voxels[span, :].astype(f32)
        for h in range(mp_n):
            after += dot(dot(hit, answers[h]).astype(bf16), w_out[h])
        normed = normalize(after, gain[...]).astype(bf16)
        hidden = jax.nn.gelu(dot(normed, w_up[...]), approximate=True).astype(bf16)
        terms = dot(hidden, w_down[...])
        mine[span, :] = pick(after, m, mp_n) + pick(terms, m, mp_n)
        for p in range(1, mp_n):
            sendbuf[p - 1, span, :] = pick(terms, (m + p) % mp_n, mp_n).astype(bf16)

        @pl.when(b > 0)
        def _():
            for p in range(1, mp_n):
                copy(b - 1, p).start()

        return carry

    lax.fori_loop(0, steps, work, 0)
    for p in range(1, mp_n):
        copy(steps - 1, p).start()

    def finish(b, carry):
        span = pl.ds(b * block, block)
        out = mine[span, :]
        for p in range(1, mp_n):
            copy(b, p).wait()
            out += recvbuf[p - 1, span, :].astype(f32)
        result[span, :] = out.astype(bf16)
        return carry

    lax.fori_loop(0, steps, finish, 0)


def ffn(mp_n, voxels, index, answers, w_out, gain, w_up, w_down):
    rows, width = voxels.shape
    part = width // mp_n
    block = math.gcd(rows, 256)
    dma = pltpu.SemaphoreType.DMA
    side = rows // block * (mp_n - 1)
    return pl.pallas_call(
        functools.partial(ffn_kernel, mp_n, block),
        out_shape=jax.ShapeDtypeStruct((rows, part), bf16),
        in_specs=[VMEM] * 7,
        out_specs=VMEM,
        scratch_shapes=[
            pltpu.VMEM((mp_n - 1, rows, part), bf16),
            pltpu.VMEM((mp_n - 1, rows, part), bf16),
            pltpu.VMEM((rows, part), f32),
            dma((side,)), dma((side,)),
        ],
        compiler_params=pltpu.CompilerParams(collective_id=2, has_side_effects=True),
        name="ffn",
    )(voxels, index, answers, w_out, gain, w_up, w_down)


def shards(
    subs,
    voxels,
    window_ids,
    voxel_slots,
    window_counts,
    norm_gain,
    w_query_key,
    w_value,
    w_out,
    ffn_gain,
    w_up,
    w_down,
):
    owners = lax.axis_size(("space", "sub"))
    my_index = lax.axis_index(("space", "sub"))
    mp_n = lax.axis_size("mp")
    rows, width = voxels.shape
    cap = 2 * rows // owners
    part = width // mp_n
    normed = normalize(voxels.astype(f32), norm_gain).astype(bf16)
    half = lax.dynamic_slice_in_dim(normed, lax.axis_index("mp") * part, part, 1)
    destination = window_ids // WIN_DEV
    position = window_ids % WIN_DEV * WLEN + voxel_slots
    target = (jnp.arange(owners, dtype=jnp.int32)[:, None] == destination[None, :]).astype(
        jnp.int32
    )
    before = jnp.sum((jnp.cumsum(target, axis=1) - target) * target, axis=0)
    send_index = destination * cap + before
    digits = jnp.stack(
        [position // BASE, position % BASE, jnp.ones_like(position)]
        + [jnp.zeros_like(position)] * 5
    ).astype(bf16)
    arrived, spots, whole_out = dispatch(
        owners, subs, mp_n, cap, half, send_index[None, :], digits, w_out
    )
    counts = lax.dynamic_slice_in_dim(window_counts, my_index * WIN_DEV, WIN_DEV, 0)
    mixture = attend(
        counts, spots.reshape(1, owners * cap), arrived.reshape(mp_n, owners * cap, part),
        w_query_key, w_value,
    )
    answers = answer(owners, subs, mp_n, cap, mixture, spots.reshape(owners, cap, 1))
    return ffn(
        mp_n, voxels, send_index[:, None],
        answers.reshape(mp_n, owners * cap, answers.shape[-1]),
        whole_out, ffn_gain[None, :], w_up, w_down,
    )


def solution(mesh):
    return jax.shard_map(
        functools.partial(shards, mesh.shape["sub"]),
        mesh=mesh,
        in_specs=(
            P(("groups", "space", "sub"), None),
            P(("groups", "space", "sub")),
            P(("groups", "space", "sub")),
            P("groups"),
            P(),
            P(None, None, "mp"),
            P(None, "mp"),
            P("mp", None),
            P(),
            P(None, "mp"),
            P("mp", None),
        ),
        out_specs=P(("groups", "space", "sub"), "mp"),
        check_vma=False,
    )
```

```python
import functools
import math

import jax
import jax.numpy as jnp
from jax import lax
from jax.experimental import pallas as pl
from jax.experimental.pallas import tpu as pltpu
from jax.sharding import PartitionSpec as P

HDIM = 64
WLEN = 256
WIN_DEV = 16
BASE = 64
MESH = pl.DeviceIdType.MESH
VMEM = pl.BlockSpec(memory_space=pltpu.VMEM)
f32 = jnp.float32
bf16 = jnp.bfloat16


def normalize(values_in, gain):
    row_mean = jnp.mean(values_in, axis=-1, keepdims=True)
    centred = values_in - row_mean
    variance = jnp.mean(centred * centred, axis=-1, keepdims=True)
    return centred * lax.rsqrt(variance + 1e-05) * gain


def iota(shape, dim):
    return lax.broadcasted_iota(jnp.int32, shape, dim)


def one_hot(found):
    return jnp.where(found, f32(1), f32(0)).astype(bf16)


def dot(a, b, dims=((1,), (0,))):
    return lax.dot_general(a, b, (dims, ((), ())), preferred_element_type=f32)


def greet(owners, subs, mp_n, me, m):
    barrier = pltpu.get_barrier_semaphore()
    for k in range(1, owners):
        t = (me + k) % owners
        pl.semaphore_signal(
            barrier, inc=1, device_id={"space": t // subs, "sub": t % subs}, device_id_type=MESH
        )
    for p in range(1, mp_n):
        pl.semaphore_signal(
            barrier, inc=1, device_id={"mp": (m + p) % mp_n}, device_id_type=MESH
        )
    pl.semaphore_wait(barrier, owners - 1 + mp_n - 1)


def to_owner(src, dst, sems, slot, target, subs):
    return pltpu.make_async_remote_copy(
        src_ref=src,
        dst_ref=dst,
        send_sem=sems[0].at[slot],
        recv_sem=sems[1].at[slot],
        device_id={"space": target // subs, "sub": target % subs},
        device_id_type=MESH,
    )


def to_mp(src, dst, sems, index, peer):
    return pltpu.make_async_remote_copy(
        src_ref=src,
        dst_ref=dst,
        send_sem=sems[0].at[index],
        recv_sem=sems[1].at[index],
        device_id={"mp": peer},
        device_id_type=MESH,
    )


def dispatch_kernel(
    spaces, subs, mp_n, normed, index, digits, out_rows, padded, spots, whole_out,
    outbuf, nearbuf, arrived, spotbuf, ms, mr, ps, pr, ss, sr, ws, wr,
):
    owners = spaces * subs
    far = owners - subs
    sp, sb, m = lax.axis_index("space"), lax.axis_index("sub"), lax.axis_index("mp")
    me = sp * subs + sb
    cap, part, rows = outbuf.shape[1], outbuf.shape[2], normed.shape[0]
    greet(owners, subs, mp_n, me, m)
    for p in range(1, mp_n):
        to_mp(out_rows, whole_out.at[m], (ws, wr), p - 1, (m + p) % mp_n).start()
    whole_out[m] = out_rows[...]

    def sink(slot):
        return (sp + slot // subs + 1) % spaces * subs + (sb + slot % subs) % subs

    def source(slot):
        return (sp + spaces - slot // subs - 1) % spaces * subs + (sb + subs - slot % subs) % subs

    def find(slot, t):
        hit = one_hot(index[...] == iota((cap, rows), 0) + t * cap)
        parts = dot(digits[...], hit, ((1,), (1,)))
        place = parts[0:1] * BASE + parts[1:2] + (1 - parts[2:3]) * (WIN_DEV * WLEN)
        spotbuf[slot] = place.astype(jnp.int32)
        return hit

    def spot_copy(slot, s, t):
        return to_owner(spotbuf.at[slot], spots.at[s], (ps, pr), slot, t, subs)

    def far_copy(slot, s, t):
        return to_owner(outbuf.at[slot], arrived.at[s, m], (ms, mr), slot, t, subs)

    def near_copy(j, s, t):
        return to_owner(nearbuf.at[j], arrived.at[s], (ms, mr), far + j, t, subs)

    def side_copy(slot, p, half, s):
        return to_mp(
            arrived.at[s, m], arrived.at[s, half], (ss, sr), slot * (mp_n - 1) + p - 1,
            (m + p) % mp_n,
        )

    def send(slot):
        far_copy(slot, me, sink(slot)).start()
        spot_copy(slot, me, sink(slot)).start()

    def build(slot, carry):
        hit = find(slot, sink(slot))
        mine = normed[:, pl.ds(pl.multiple_of(m * part, part), part)]
        outbuf[slot] = dot(hit, mine).astype(bf16)

        @pl.when(slot > 0)
        def _():
            send(slot - 1)

        return carry

    lax.fori_loop(0, far, build, 0)
    for j in range(subs):
        hit = find(far + j, sp * subs + (sb + j) % subs)
        for h in range(mp_n):
            nearbuf[j, h] = dot(hit, normed[:, h * part : (h + 1) * part]).astype(bf16)
        if j == 0:
            send(far - 1)
        elif j > 1:
            near_copy(j - 1, me, sp * subs + (sb + j - 1) % subs).start()
            spot_copy(far + j - 1, me, sp * subs + (sb + j - 1) % subs).start()
    spots[me] = spotbuf[far]
    chunk = 4 * WLEN

    def put(s, blocks, first):
        row = spots[s]

        def span(c, carry):
            hit = one_hot(row == iota((chunk, cap), 0) + c * chunk)
            here = pl.ds(c * chunk, chunk)
            for h in range(mp_n):
                new = dot(hit, blocks[h]).astype(bf16)
                if not first:
                    new += padded[here, h * part : (h + 1) * part]
                padded[here, h * part : (h + 1) * part] = new
            return carry

        lax.fori_loop(0, padded.shape[0] // chunk, span, 0)

    put(me, nearbuf.at[0], True)
    for j in range(max(subs - 1, 1), subs):
        near_copy(j, me, sp * subs + (sb + j) % subs).start()
        spot_copy(far + j, me, sp * subs + (sb + j) % subs).start()

    def settle(slot):
        s = source(slot)
        for p in range(1, mp_n):
            side_copy(slot, p, (m + mp_n - p) % mp_n, s).wait()
        spot_copy(slot, s, s).wait()
        put(s, arrived.at[s], False)

    def onward(slot, carry):
        s = source(slot)
        far_copy(slot, s, s).wait()
        for p in range(1, mp_n):
            side_copy(slot, p, m, s).start()

        @pl.when(slot > 0)
        def _():
            settle(slot - 1)

        return carry

    lax.fori_loop(0, far, onward, 0)
    for j in range(1, subs):
        s = sp * subs + (sb + subs - j) % subs
        near_copy(j, s, s).wait()
        spot_copy(far + j, s, s).wait()
        put(s, arrived.at[s], False)
    settle(far - 1)
    for p in range(1, mp_n):
        to_mp(
            out_rows, whole_out.at[(m + mp_n - p) % mp_n], (ws, wr), p - 1, (m + p) % mp_n
        ).wait()


def dispatch(spaces, subs, mp_n, cap, normed, index, digits, out_rows):
    owners = spaces * subs
    width = normed.shape[1]
    part = width // mp_n
    dma = pltpu.SemaphoreType.DMA
    side = owners * (mp_n - 1)
    return pl.pallas_call(
        functools.partial(dispatch_kernel, spaces, subs, mp_n),
        out_shape=(
            jax.ShapeDtypeStruct((WIN_DEV * WLEN, width), bf16),
            jax.ShapeDtypeStruct((owners, 1, cap), jnp.int32),
            jax.ShapeDtypeStruct((mp_n,) + out_rows.shape, bf16),
        ),
        in_specs=[VMEM] * 4,
        out_specs=(VMEM, VMEM, VMEM),
        scratch_shapes=[
            pltpu.VMEM((owners - subs, cap, part), bf16),
            pltpu.VMEM((subs, mp_n, cap, part), bf16),
            pltpu.VMEM((owners, mp_n, cap, part), bf16),
            pltpu.VMEM((owners, 1, cap), jnp.int32),
            dma((owners,)), dma((owners,)), dma((owners,)), dma((owners,)),
            dma((side,)), dma((side,)), dma((mp_n,)), dma((mp_n,)),
        ],
        compiler_params=pltpu.CompilerParams(collective_id=0, has_side_effects=True),
        name="dispatch",
    )(normed, index, digits, out_rows)


def attend_kernel(group, counts, padded, w_qk, w_v, mixture):
    step = pl.program_id(0)
    local = w_v.shape[1]
    heads = local // HDIM
    rows_in = padded[...]
    queries = dot(rows_in, w_qk[0]).astype(bf16)
    keys = dot(rows_in, w_qk[1]).astype(bf16)
    values = dot(rows_in, w_v[...]).astype(bf16)
    head_of = iota((1, local), 1) // HDIM
    masks = [jnp.where(head_of == h, f32(1), f32(0)).astype(bf16) for h in range(heads)]
    for g in range(group):
        span = slice(g * WLEN, (g + 1) * WLEN)
        q, k, v = queries[span], keys[span], values[span]
        stacked = jnp.concatenate([q * masks[h] for h in range(heads)], axis=0)
        scores = dot(stacked, k, ((1,), (1,))) * f32(HDIM ** -0.5)
        live = iota((1, WLEN), 1) < counts[step * group + g]
        scores = jnp.where(live, scores, f32(-1e30))
        weights = jnp.exp(scores - jnp.max(scores, axis=-1, keepdims=True))
        scale = 1.0 / jnp.sum(weights, axis=-1, keepdims=True)
        mixed = dot((weights * scale).astype(bf16), v)
        out = mixed[:WLEN]
        for h in range(1, heads):
            out = jnp.where(head_of == h, mixed[h * WLEN : (h + 1) * WLEN], out)
        mixture[span, :] = out.astype(bf16)


def attend(counts, padded, w_qk, w_v, group=2):
    local = w_v.shape[1]
    slots = group * WLEN
    whole = lambda a: pl.BlockSpec(a.shape, lambda i: (0,) * a.ndim)
    return pl.pallas_call(
        functools.partial(attend_kernel, group),
        grid=(WIN_DEV // group,),
        out_shape=jax.ShapeDtypeStruct((WIN_DEV * WLEN, local), bf16),
        in_specs=[
            pl.BlockSpec(memory_space=pltpu.SMEM),
            pl.BlockSpec((slots, padded.shape[1]), lambda i: (i, 0)),
            whole(w_qk),
            whole(w_v),
        ],
        out_specs=pl.BlockSpec((slots, local), lambda i: (i, 0)),
        name="attend",
    )(counts, padded, w_qk, w_v)


def answer_kernel(
    owners, subs, mp_n, mixture, column, index, attended, outbuf, answers, total, ms, mr, ss, sr
):
    me = lax.axis_index("space") * subs + lax.axis_index("sub")
    m = lax.axis_index("mp")
    cap, local = outbuf.shape[1], outbuf.shape[2]
    rows = index.shape[0]
    span = 4 * WLEN
    greet(owners, subs, mp_n, me, m)

    def main_copy(slot, s, t):
        return to_owner(outbuf.at[slot], answers.at[m, s], (ms, mr), slot, t, subs)

    def side_copy(slot, p, src, half, s):
        return to_mp(
            src, answers.at[half, s], (ss, sr), slot * (mp_n - 1) + p - 1, (m + p) % mp_n
        )

    def send(slot):
        t = (me + slot) % owners

        @pl.when(slot > 0)
        def _():
            main_copy(slot, me, t).start()

        @pl.when(slot == 0)
        def _():
            for p in range(1, mp_n):
                side_copy(0, p, outbuf.at[0], m, me).start()

    def onward(slot, carry):
        s = (me + owners - slot) % owners
        main_copy(slot, s, s).wait()
        for p in range(1, mp_n):
            side_copy(slot, p, answers.at[m, s], m, s).start()
        return carry

    def build(slot, carry):
        place = column[(me + slot) % owners]
        total[...] = jnp.zeros_like(total)

        def add(c, inner):
            hit = one_hot(place == iota((cap, span), 1) + c * span)
            total[...] += dot(hit, mixture[pl.ds(c * span, span), :])
            return inner

        lax.fori_loop(0, mixture.shape[0] // span, add, 0)
        outbuf[slot] = total[...].astype(bf16)

        @pl.when(slot > 0)
        def _():
            send(slot - 1)

        @pl.when((slot >= 4) & (slot % 2 == 0))
        def _():
            onward(slot // 2 - 1, 0)

        return carry

    lax.fori_loop(0, owners, build, 0)
    send(owners - 1)
    answers[m, me] = outbuf[0]
    attended[...] = jnp.zeros_like(attended)

    def settle(slot):
        s = (me + owners - slot) % owners
        for p in range(1, mp_n):
            side_copy(slot, p, outbuf.at[slot], (m + mp_n - p) % mp_n, s).wait()
        hit = one_hot(index[...] == iota((rows, cap), 1) + s * cap)
        for h in range(mp_n):
            attended[h] += dot(hit, answers[h, s]).astype(bf16)

    ahead = max((owners - 1) // 2 - 1, 0)

    def drain(slot, carry):
        onward(slot, 0)
        settle(slot - ahead - 1)
        return carry

    lax.fori_loop(ahead + 1, owners, drain, 0)

    def rest(slot, carry):
        settle(slot)
        return carry

    lax.fori_loop(owners - ahead - 1, owners, rest, 0)


def answer(owners, subs, mp_n, cap, mixture, column, index):
    local = mixture.shape[1]
    dma = pltpu.SemaphoreType.DMA
    side = owners * (mp_n - 1)
    return pl.pallas_call(
        functools.partial(answer_kernel, owners, subs, mp_n),
        out_shape=jax.ShapeDtypeStruct((mp_n, index.shape[0], local), bf16),
        in_specs=[VMEM] * 3,
        out_specs=VMEM,
        scratch_shapes=[
            pltpu.VMEM((owners, cap, local), bf16),
            pltpu.VMEM((mp_n, owners, cap, local), bf16),
            pltpu.VMEM((cap, local), f32),
            dma((owners,)), dma((owners,)), dma((side,)), dma((side,)),
        ],
        compiler_params=pltpu.CompilerParams(collective_id=1, has_side_effects=True),
        name="answer",
    )(mixture, column, index)


def pick(value, which, pieces):
    part = value.shape[1] // pieces
    out = value[:, :part]
    for j in range(1, pieces):
        out = jnp.where(which == j, value[:, j * part : (j + 1) * part], out)
    return out


def ffn_kernel(
    mp_n, block, voxels, attended, w_out, gain, w_up, w_down, result,
    sendbuf, recvbuf, mine, ss, sr,
):
    m = lax.axis_index("mp")
    rows = voxels.shape[0]
    steps = rows // block
    barrier = pltpu.get_barrier_semaphore()
    for p in range(1, mp_n):
        pl.semaphore_signal(
            barrier, inc=1, device_id={"mp": (m + p) % mp_n}, device_id_type=MESH
        )
    pl.semaphore_wait(barrier, mp_n - 1)

    def copy(b, p):
        span = pl.ds(b * block, block)
        return to_mp(
            sendbuf.at[p - 1, span], recvbuf.at[p - 1, span], (ss, sr),
            b * (mp_n - 1) + p - 1, (m + p) % mp_n,
        )

    def work(b, carry):
        span = pl.ds(b * block, block)
        after = voxels[span, :].astype(f32)
        for h in range(mp_n):
            after += dot(attended[h, span, :], w_out[h])
        normed = normalize(after, gain[...]).astype(bf16)
        hidden = jax.nn.gelu(dot(normed, w_up[...]), approximate=True).astype(bf16)
        terms = dot(hidden, w_down[...])
        mine[span, :] = pick(after, m, mp_n) + pick(terms, m, mp_n)
        for p in range(1, mp_n):
            sendbuf[p - 1, span, :] = pick(terms, (m + p) % mp_n, mp_n).astype(bf16)

        @pl.when(b > 0)
        def _():
            for p in range(1, mp_n):
                copy(b - 1, p).start()

        return carry

    lax.fori_loop(0, steps, work, 0)
    for p in range(1, mp_n):
        copy(steps - 1, p).start()

    def finish(b, carry):
        span = pl.ds(b * block, block)
        out = mine[span, :]
        for p in range(1, mp_n):
            copy(b, p).wait()
            out += recvbuf[p - 1, span, :].astype(f32)
        result[span, :] = out.astype(bf16)
        return carry

    lax.fori_loop(0, steps, finish, 0)


def ffn(mp_n, voxels, attended, w_out, gain, w_up, w_down):
    rows, width = voxels.shape
    part = width // mp_n
    block = math.gcd(rows, 256)
    dma = pltpu.SemaphoreType.DMA
    side = rows // block * (mp_n - 1)
    return pl.pallas_call(
        functools.partial(ffn_kernel, mp_n, block),
        out_shape=jax.ShapeDtypeStruct((rows, part), bf16),
        in_specs=[VMEM] * 6,
        out_specs=VMEM,
        scratch_shapes=[
            pltpu.VMEM((mp_n - 1, rows, part), bf16),
            pltpu.VMEM((mp_n - 1, rows, part), bf16),
            pltpu.VMEM((rows, part), f32),
            dma((side,)), dma((side,)),
        ],
        compiler_params=pltpu.CompilerParams(collective_id=2, has_side_effects=True),
        name="ffn",
    )(voxels, attended, w_out, gain, w_up, w_down)


def shards(
    subs,
    voxels,
    window_ids,
    voxel_slots,
    window_counts,
    norm_gain,
    w_query_key,
    w_value,
    w_out,
    ffn_gain,
    w_up,
    w_down,
):
    owners = lax.axis_size(("space", "sub"))
    my_index = lax.axis_index(("space", "sub"))
    mp_n = lax.axis_size("mp")
    rows = voxels.shape[0]
    cap = 2 * rows // owners
    normed = normalize(voxels.astype(f32), norm_gain).astype(bf16)
    destination = window_ids // WIN_DEV
    position = window_ids % WIN_DEV * WLEN + voxel_slots
    target = (jnp.arange(owners, dtype=jnp.int32)[:, None] == destination[None, :]).astype(
        jnp.int32
    )
    before = jnp.sum((jnp.cumsum(target, axis=1) - target) * target, axis=0)
    send_index = destination * cap + before
    digits = jnp.stack(
        [position // BASE, position % BASE, jnp.ones_like(position)]
        + [jnp.zeros_like(position)] * 5
    ).astype(bf16)
    padded, spots, whole_out = dispatch(
        owners // subs, subs, mp_n, cap, normed, send_index[None, :], digits, w_out
    )
    counts = lax.dynamic_slice_in_dim(window_counts, my_index * WIN_DEV, WIN_DEV, 0)
    mixture = attend(counts, padded, w_query_key, w_value)
    attended = answer(
        owners, subs, mp_n, cap, mixture, spots.reshape(owners, cap, 1), send_index[:, None]
    )
    return ffn(mp_n, voxels, attended, whole_out, ffn_gain[None, :], w_up, w_down)


def solution(mesh):
    return jax.shard_map(
        functools.partial(shards, mesh.shape["sub"]),
        mesh=mesh,
        in_specs=(
            P(("groups", "space", "sub"), None),
            P(("groups", "space", "sub")),
            P(("groups", "space", "sub")),
            P("groups"),
            P(),
            P(None, None, "mp"),
            P(None, "mp"),
            P("mp", None),
            P(),
            P(None, "mp"),
            P("mp", None),
        ),
        out_specs=P(("groups", "space", "sub"), "mp"),
        check_vma=False,
    )
```
